32 devices in a mesh: seq: 8 (over z, y), head: 4 (over x, core).
Axes of the slice: x: 2, y: 2, z: 4, core: 2. Of those that a mesh axis runs over, the one named last changes fastest.
Arguments:
- queries: bfloat16 [1024, 4096], P('seq', 'head'), may hold values from -40 to 40
- keys: bfloat16 [1024, 512], P(('seq', 'head')), may hold values from -40 to 40
- values: bfloat16 [1024, 512], P(('seq', 'head')), may hold values from -6 to 6
- block_order: int32 [8], replicated, may hold values from 0 to 7, each once
Outputs:
- attended: bfloat16 [1024, 4096], P('seq', 'head')
The draws below stay inside these ranges and needn't reach their ends.
All inputs are finite; a program needn't handle non-finite values.
Results may differ from the reference program's by a relative error of at most 0.0055.
Values may be sent and summed in bfloat16 or wider, within the bound.
A program may use at most 64 MiB of HBM per device.

```python
import math
import jax
import jax.numpy as jnp
from jax import lax

HD = 128
QH = 32
KVH = 4
TOK_DEV = 128
GROUP = 8
TOKENS = 1024
N_SEQ = 8


def joint_draw(key):
    base = jax.random.fold_in(key, 11)
    key_query, key_key = jax.random.split(base, 2)
    query_part = jax.random.normal(key_query, (TOKENS, KVH, GROUP, HD), jnp.float32)
    key_part = jax.random.normal(key_key, (TOKENS, KVH, HD), jnp.float32)
    query_part = jnp.clip(query_part, -40.0, 40.0)
    key_part = jnp.clip(key_part, -40.0, 40.0)
    return (query_part.reshape(TOKENS, QH * HD), key_part.reshape(TOKENS, KVH * HD))


def draw_queries(key, part):
    return joint_draw(key)[0].astype(jnp.bfloat16)


def draw_keys(key, part):
    return joint_draw(key)[1].astype(jnp.bfloat16)


def levels(own_key, extent, shards, low, high):
    def one(axis_at, shards_of):
        heights = jax.random.uniform(jax.random.fold_in(jax.random.fold_in(own_key, 6), axis_at), (shards_of,), jnp.float32, low / len(shards), high / len(shards))
        return jnp.repeat(jnp.exp(heights), extent[axis_at] // shards_of).reshape((-1,) + (1,) * (len(extent) - axis_at - 1))

    loudness = one(*shards[0])
    for cut in shards[1:]:
        loudness = loudness * one(*cut)
    return loudness


def gaussian(own_key, extent, width, reach, shards=(), held_as=jnp.bfloat16):
    factor_of = levels(own_key, extent, shards, -0.22, 0.18) if shards else 1.0
    values = jax.random.normal(own_key, extent, jnp.float32) * width * factor_of
    return jnp.minimum(jnp.maximum(values, -reach), reach).astype(held_as)


def setup_inputs(seed: int = 0) -> dict:
    seeds = jax.random.split(jax.random.key(seed), 5)
    return {
        "queries": draw_queries(jax.random.fold_in(seeds[4], 71), 0),
        "keys": draw_keys(jax.random.fold_in(seeds[4], 71), 0),
        "values": gaussian(seeds[2], (TOKENS, KVH * HD), 1.0, 6.0, ((0, 32),)),
        "block_order": jax.random.permutation(seeds[3], N_SEQ).astype(jnp.int32),
    }


def reference(queries, keys, values, block_order):
    position = (block_order[:, None] * TOK_DEV + jnp.arange(TOK_DEV, dtype=jnp.int32)[None, :]).reshape(-1).astype(jnp.int32)
    query_heads = queries.reshape(TOKENS, KVH, GROUP, HD)
    key_heads = keys.reshape(TOKENS, KVH, HD)
    value_heads = values.reshape(TOKENS, KVH, HD)
    row_block = math.gcd(TOKENS, 512)
    factor = 1.0 / math.sqrt(HD)

    def per_head(head_index):
        key_cols = lax.dynamic_index_in_dim(key_heads, head_index, 1, keepdims=False).astype(jnp.float32)
        value_cols = lax.dynamic_index_in_dim(value_heads, head_index, 1, keepdims=False).astype(jnp.float32)
        query_cols = lax.dynamic_index_in_dim(query_heads, head_index, 1, keepdims=False)

        def per_block(block_index):
            start = (block_index * row_block).astype(jnp.int32)
            query_rows = lax.dynamic_slice_in_dim(query_cols, start, row_block, 0).astype(jnp.float32)
            query_pos = lax.dynamic_slice_in_dim(position, start, row_block, 0)
            scores = jnp.einsum('qgd,kd->gqk', query_rows, key_cols) * factor
            visible = (query_pos[:, None] >= position[None, :])[None]
            scores = jnp.where(visible, scores, -1e+30)
            highest = lax.optimization_barrier(jnp.max(scores, axis=-1, keepdims=True))
            weights = jnp.where(visible, jnp.exp(scores - highest), 0.0)
            totals = lax.optimization_barrier(jnp.sum(weights, axis=-1))
            rounded = lax.optimization_barrier(weights.astype(jnp.bfloat16)).astype(jnp.float32)
            numerator = jnp.einsum('gqk,kd->qgd', rounded, value_cols)
            return numerator / jnp.transpose(totals)[:, :, None]
        result = lax.map(per_block, jnp.arange(TOKENS // row_block, dtype=jnp.int32))
        return result.reshape(TOKENS, GROUP, HD)
    every = lax.map(per_head, jnp.arange(KVH, dtype=jnp.int32))
    return jnp.transpose(every, (1, 0, 2, 3)).reshape(TOKENS, QH * HD).astype(jnp.bfloat16)
```

```python
import functools
import math

import jax
import jax.numpy as jnp
from jax import lax
from jax.experimental import pallas as pl
from jax.experimental.pallas import tpu as pltpu
from jax.sharding import PartitionSpec as P

HD = 128
NEG = -1e30
MESH = pl.DeviceIdType.MESH
DD=9
LAST=[0,2,1]
HORD=0
SPLIT=2


def kernel(
    outer, inner, heads,
    order_hbm, q_hbm, k_hbm, v_hbm, acc, total,
    order, q_ref, kvd, high,
    load_sem, ready, near, sent, recv,
):
    rows = k_hbm.shape[0]
    block = q_ref.shape[0]
    width = kvd.shape[-1]
    q_heads = q_ref.shape[1] // HD
    seq, head = lax.axis_index("seq"), lax.axis_index("head")
    o, j = seq // inner, lax.rem(seq, inner)
    place = pl.ds(pl.multiple_of(head * rows, rows), rows)
    far = min(DD, outer)
    halves = SPLIT
    per_half = heads // halves
    chunk = rows * per_half
    mine_half = head // per_half

    def order_of(t):
        if HORD == 0:
            return t
        if HORD == 1:
            return lax.rem(head + t, heads)
        if HORD == 2:
            return jnp.bitwise_xor(head, t)
        if HORD == 3:
            return jnp.bitwise_xor(head, heads - 1 - t)

    def loop(first, last, body):
        lax.fori_loop(first, last, lambda k, c: (body(k), c)[1], 0)

    def columns(h):
        return pl.ds(pl.multiple_of(h * width, width), width)

    def lane(dj):
        return lax.rem(j + dj, inner)

    def signal(sem, o2, j2, h2):
        pl.semaphore_signal(sem, inc=1, device_id=(o2 * inner + j2, h2), device_id_type=MESH)

    under, above = (0, o), (o + 1, outer)
    deep, high_up = (0, jnp.maximum(o - far + 1, 0)), (jnp.minimum(o + far, outer), outer)
    spot, spots = j * heads + head, inner * heads

    barrier = pltpu.get_barrier_semaphore()

    def greet(dj):
        def body(o2):
            for h2 in range(heads):
                signal(barrier, o2, lane(dj), h2)
        return body

    loop(spot + 1, spots, lambda t: signal(barrier, o, t // heads, lax.rem(t, heads)))
    loop(*above, greet(0))
    for dj in range(1, inner):
        loop(*high_up, greet(dj))
    own = [
        pltpu.make_async_copy(src.at[:, columns(head)], kvd.at[o, j, i, place], load_sem.at[0])
        for i, src in enumerate((k_hbm, v_hbm))
    ]
    qload = pltpu.make_async_copy(q_hbm, q_ref, load_sem.at[1])
    oload = pltpu.make_async_copy(order_hbm, order, load_sem.at[2])
    for c in own + [qload, oload]:
        c.start()

    ahead = spot + o * heads + deep[1] * (inner - 1) * heads
    pl.when(ahead > 0)(lambda: pl.semaphore_wait(barrier, ahead))

    def piece(o2, j2, h2):
        for i, src in enumerate((k_hbm, v_hbm)):
            pltpu.make_async_remote_copy(
                src_ref=src.at[:, columns(h2)],
                dst_ref=kvd.at[o, j, i, place],
                send_sem=sent.at[o2],
                recv_sem=recv.at[o, j, mine_half],
                device_id=(o2 * inner + j2, h2),
                device_id_type=MESH,
            ).start()

    def push(dj):
        def body(o2):
            for t in range(heads):
                piece(o2, lane(dj), order_of(t))
        return body

    def tell(dj):
        def body(o2):
            for h2 in range(heads):
                signal(ready.at[o], o2, lane(dj), h2)
        return body

    for dj in range(1, inner):
        loop(*deep, push(dj))
    loop(*under, push(0))
    loop(0, spot, lambda t: piece(o, t // heads, lax.rem(t, heads)))
    loop(0, spot, lambda t: signal(near.at[j], o, t // heads, lax.rem(t, heads)))
    for dj in range(1, inner):
        loop(*deep, tell(dj))
    loop(*under, tell(0))

    def neighbours(j2):
        first = jnp.maximum(spot + 1 - j2 * heads, 0)
        pl.when(first < heads)(lambda: pl.semaphore_wait(near.at[j2], heads - first))
        loop(first, heads, lambda h2: piece(o, j2, h2))

    loop(j, inner, neighbours)

    def upward(o2):
        wide = jnp.minimum(jnp.maximum(o2 - o - far + 1, 0), 1) * (inner - 1) + 1
        pl.semaphore_wait(ready.at[o2], wide * heads)

        def lanes_of(dj):
            for t in range(heads):
                piece(o2, lane(dj), order_of(t))

        loop(0, wide, lanes_of)

    loop(*above, upward)

    mine_part = kvd.at[0, 0, :, pl.ds(0, rows)]
    whole = kvd.at[0, 0, :, pl.ds(0, chunk)]
    part = kvd.at[0, 0, :, pl.ds(0, chunk - rows)]

    def other_half(f):
        return lax.rem(mine_half + f, halves)

    def landed(src, dj):
        for f in range(halves):
            pltpu.make_async_copy(whole, whole, recv.at[src, lane(dj), other_half(f)]).wait()

    def relay(src):
        for f in range(halves):
            part_of = other_half(f)
            pltpu.make_async_copy(whole, whole, recv.at[src, j, part_of]).wait()
            piece_of = kvd.at[src, j, :, pl.ds(pl.multiple_of(part_of * chunk, chunk), chunk)]

            def pass_on(dj, piece_of=piece_of, part_of=part_of):
                pltpu.make_async_remote_copy(
                    src_ref=piece_of,
                    dst_ref=piece_of,
                    send_sem=sent.at[src],
                    recv_sem=recv.at[src, j, part_of],
                    device_id=(o * inner + lane(dj), head),
                    device_id_type=MESH,
                ).start()

            pl.when(jnp.abs(src - o) < far)(lambda: [pass_on(dj) for dj in range(1, inner)] and None)

    half = max(outer // 2, 1)
    turned = jnp.minimum(o // half, 1)
    seen_from = o + turned * (outer - 1 - 2 * o)

    def source(i):
        a = i + (i + outer - seen_from) // outer
        return a + turned * (outer - 1 - 2 * a)

    factor = math.log2(math.e) / math.sqrt(HD)
    per = 2 if q_heads % 2 == 0 else 1
    lanes = per * block

    def absorb(src, dj, first=False):
        l = lane(dj)
        if first:
            row = lax.broadcasted_iota(jnp.int32, (block, lanes), 0)
            col = lax.broadcasted_iota(jnp.int32, (block, lanes), 1)
            visible = lax.rem(col, block) >= row
        else:
            seen = jnp.full((1, lanes), order[src * inner + l], jnp.int32) < order[seq]
        key = kvd[src, l, 0]
        value = kvd[src, l, 1]
        for c in range(q_heads // per):
            q = jnp.concatenate(
                [q_ref[:, (c * per + i) * HD : (c * per + i + 1) * HD] for i in range(per)], axis=0
            )
            s = lax.dot_general(key, q, (((1,), (1,)), ((), ())), preferred_element_type=jnp.float32)
            s = s * factor
            if first:
                s = jnp.where(visible, s, NEG)
            cols = slice(c * lanes, (c + 1) * lanes)
            top = jnp.max(s, axis=0, keepdims=True)
            if first:
                p = jnp.exp2(s - top)
                high[:, cols] = top
            else:
                old = high[:, cols]
                top = jnp.where(seen, jnp.maximum(old, top), old)
                p = jnp.exp2(s - jnp.where(seen, top, -NEG))
                high[:, cols] = top
            t = jnp.sum(p, axis=0, keepdims=True)
            pv = lax.dot_general(
                value, p.astype(jnp.bfloat16), (((0,), (0,)), ((), ())), preferred_element_type=jnp.float32
            )
            if first:
                total[:, cols] = t
                acc[:, cols] = pv
            else:
                scale = jnp.exp2(old - top)
                total[:, cols] = total[:, cols] * scale + t
                acc[:, cols] = acc[:, cols] * scale + pv

    qload.wait()
    oload.wait()
    pltpu.make_async_copy(mine_part, mine_part, load_sem.at[0]).wait()
    pltpu.make_async_copy(part, part, recv.at[o, j, mine_half]).wait()
    for f in range(1, halves):
        pltpu.make_async_copy(whole, whole, recv.at[o, j, other_half(f)]).wait()
    absorb(o, 0, True)

    def across(src):
        for dj in range(1, inner):
            landed(src, dj)
            absorb(src, dj)

    if outer == 1:
        across(o)
    elif outer <= 8:
        srcs = [source(i) for i in range(outer - 1)]
        relay(srcs[0])
        across(o)
        absorb(srcs[0], 0)
        for src in srcs[1:]:
            relay(src)
            absorb(src, 0)
        for i in LAST if outer == 4 else range(outer - 1):
            across(srcs[i])
    else:
        across(o)

        def further(i):
            src = source(i)
            relay(src)
            absorb(src, 0)
            across(src)

        loop(0, outer - 1, further)

    most = kvd.at[0, :, :, pl.ds(0, block - block // spots)]
    full = kvd.at[0]

    def drain(o2):
        pltpu.make_async_copy(full, full, sent.at[o2]).wait()

    loop(0, o, drain)
    pltpu.make_async_copy(most, most, sent.at[o]).wait()
    loop(o + 1, outer, drain)


def finish(acc, total, out_ref):
    block, q_cols = out_ref.shape
    for g in range(q_cols // HD):
        lane = slice(g * block, (g + 1) * block)
        part = acc[:, lane] / total[:, lane]
        out_ref[:, g * HD : (g + 1) * HD] = part.T.astype(out_ref.dtype)


def local(devices, heads, queries, keys, values, block_order):
    inner = 2 if devices % 2 == 0 else 1
    outer = devices // inner
    rows, cols = keys.shape
    block, q_cols = queries.shape
    width = cols // heads
    assert width == HD and rows * heads == block
    bf16, f32 = jnp.bfloat16, jnp.float32
    lanes = q_cols // HD * block
    acc, total = pl.pallas_call(
        functools.partial(kernel, outer, inner, heads),
        out_shape=(
            pltpu.VMEM((HD, lanes), f32),
            pltpu.VMEM((1, lanes), f32),
        ),
        in_specs=[pl.BlockSpec(memory_space=pltpu.HBM)] * 4,
        out_specs=[pl.BlockSpec(memory_space=pltpu.VMEM)] * 2,
        scratch_shapes=[
            pltpu.SMEM(block_order.shape, jnp.int32),
            pltpu.VMEM((block, q_cols), bf16),
            pltpu.VMEM((outer, inner, 2, block, width), bf16),
            pltpu.VMEM((1, lanes), f32),
            pltpu.SemaphoreType.DMA((3,)),
            pltpu.SemaphoreType.REGULAR((outer,)),
            pltpu.SemaphoreType.REGULAR((inner,)),
            pltpu.SemaphoreType.DMA((outer,)),
            pltpu.SemaphoreType.DMA((outer, inner, SPLIT)),
        ],
        compiler_params=pltpu.CompilerParams(
            collective_id=0, has_side_effects=True, vmem_limit_bytes=67043328 - 600 * 1024
        ),
    )(block_order, queries, keys, values)
    return pl.pallas_call(
        finish,
        out_shape=jax.ShapeDtypeStruct((block, q_cols), queries.dtype),
        in_specs=[pl.BlockSpec(memory_space=pltpu.VMEM)] * 2,
        out_specs=pl.BlockSpec(memory_space=pltpu.VMEM),
        compiler_params=pltpu.CompilerParams(vmem_limit_bytes=8 * 1024 * 1024),
    )(acc, total)


def solution(mesh):
    placed = (P("seq", "head"), P(("seq", "head"), None), P(("seq", "head"), None), P())
    return jax.shard_map(
        functools.partial(local, mesh.shape["seq"], mesh.shape["head"]),
        mesh=mesh, in_specs=placed, out_specs=P("seq", "head"), check_vma=False,
    )
```

```python
import functools
import math

import jax
import jax.numpy as jnp
from jax import lax
from jax.experimental import pallas as pl
from jax.experimental.pallas import tpu as pltpu
from jax.sharding import PartitionSpec as P

HD = 128
NEG = -1e30
MESH = pl.DeviceIdType.MESH
DD=9
ABS=True
PRIO=True
LATE=True
KB=600
NEARFIRST=True


FACTOR = math.log2(math.e) / math.sqrt(HD)


def attend(q, key, value, mask, old):
    s = lax.dot_general(key, q, (((1,), (1,)), ((), ())), preferred_element_type=jnp.float32)
    s = s * FACTOR
    if old is None:
        s = jnp.where(mask, s, NEG)
        top = jnp.max(s, axis=0, keepdims=True)
        p = jnp.exp2(s - top)
    else:
        block = s.shape[0] // len(mask)
        parts = [s[n * block : (n + 1) * block] for n in range(len(mask))]
        top = old[0]
        for part, shown in zip(parts, mask):
            top = jnp.where(shown, jnp.maximum(top, jnp.max(part, axis=0, keepdims=True)), top)
        p = jnp.concatenate(
            [jnp.exp2(part - jnp.where(shown, top, -NEG)) for part, shown in zip(parts, mask)]
        )
    t = jnp.sum(p, axis=0, keepdims=True)
    pv = lax.dot_general(
        value, p.astype(jnp.bfloat16), (((0,), (0,)), ((), ())), preferred_element_type=jnp.float32
    )
    if old is None:
        return top, t, pv
    scale = jnp.exp2(old[0] - top)
    return top, old[1] * scale + t, old[2] * scale + pv


def kernel(
    outer, inner, heads,
    order_hbm, q_hbm, k_hbm, v_hbm, acc, total,
    order, q_ref, kz, kvd, high,
    load_sem, ready, near, zsent, zrecv, dsent, sent, recv,
):
    rows, cols = k_hbm.shape
    block = q_ref.shape[0]
    width = kvd.shape[-1]
    q_heads = q_ref.shape[1] // HD
    seq, head = lax.axis_index("seq"), lax.axis_index("head")
    o, j = seq // inner, lax.rem(seq, inner)
    first_heads = max(heads // 2, 1)
    spots = inner * heads
    corner = (j == 0) & (head < first_heads)
    place = pl.ds(pl.multiple_of(j * block + head * rows, rows), rows)
    inputs = (k_hbm, v_hbm)

    def loop(first, last, body):
        lax.fori_loop(first, last, lambda k, c: (body(k), c)[1], 0)

    def columns(h):
        return pl.ds(pl.multiple_of(h * width, width), width)

    def lane(dj):
        return lax.rem(j + dj, inner)

    def signal(sem, o2, j2, h2):
        pl.semaphore_signal(sem, inc=1, device_id=(o2 * inner + j2, h2), device_id_type=MESH)

    barrier = pltpu.get_barrier_semaphore()

    def each_spot(js, hs, sem):
        def row(j2):
            def one(h2):
                pl.when((j2 != j) | (h2 != head))(lambda: signal(sem, o, j2, h2))
            loop(*hs, one)
        loop(*js, row)

    loop(o + 1, outer, lambda o2: signal(barrier, o2, j, head))
    each_spot((j, inner), (head, heads), barrier)

    @pl.when(corner & (o == 0))
    def _():
        def row(o2):
            for j2 in range(inner):
                for h2 in range(heads):
                    pl.when((j2 != j) | (h2 != head))(lambda: signal(barrier, o2, j2, h2))

        loop(DD, outer, row)

    own = [
        pltpu.make_async_copy(src.at[:, columns(head)], kvd.at[o, i, place], load_sem.at[0])
        for i, src in enumerate(inputs)
    ]
    qload = pltpu.make_async_copy(q_hbm, q_ref, load_sem.at[1])
    oload = pltpu.make_async_copy(order_hbm, order, load_sem.at[2])
    for c in own + [qload, oload]:
        c.start()

    ahead = o + (j + 1) * (head + 1) - 1
    extra = first_heads - jnp.where(corner, 1, 0)
    ahead = ahead + jnp.where(o >= DD, extra, 0)
    pl.when(ahead > 0)(lambda: pl.semaphore_wait(barrier, ahead))

    def zsend(o2):
        for i, src in enumerate(inputs):
            pltpu.make_async_remote_copy(
                src_ref=src,
                dst_ref=kz.at[o, i],
                send_sem=zsent.at[0],
                recv_sem=zrecv.at[o, i],
                device_id=(o2 * inner + j, head),
                device_id_type=MESH,
            ).start()

    loop(0, o, lambda o2: signal(ready.at[o], o2, j, head))

    def piece(ref, src, i, o2, j2, h2, sem):
        pltpu.make_async_remote_copy(
            src_ref=ref.at[:, columns(h2)],
            dst_ref=kvd.at[src, i, place],
            send_sem=sem,
            recv_sem=recv.at[src, j],
            device_id=(o2 * inner + j2, h2),
            device_id_type=MESH,
        ).start()

    @pl.when(o >= DD)
    def _():
        for i, ref in enumerate(inputs):
            for h2 in range(first_heads):
                pl.when((j > 0) | (head != h2))(
                    lambda: piece(ref, o, i, 0, 0, h2, dsent.at[0])
                )

    if LATE:
        loop(0, jnp.minimum(o, 1), zsend)
    else:
        loop(0, o, zsend)
    each_spot((0, j + 1), (0, head + 1), near.at[0])

    def scatter(src, i, ref, first=0, last=8):
        if ABS:
            for t in range(first, min(last, spots)):
                j2, h2 = t // heads, t % heads
                skip = (src >= DD) & (o == 0) if (j2 == 0 and h2 < first_heads) else False
                go = (j2 != j) | (h2 != head)
                if skip is not False:
                    go = go & jnp.logical_not(skip)
                pl.when(go)(lambda: piece(ref, src, i, o, j2, h2, sent.at[src]))
        else:
            group = [(dj, dh) for dj in range(inner) for dh in range(heads)][1:]
            for dj, dh in group:
                j2, h2 = lane(dj), lax.rem(head + dh, heads)
                if DD > 8:
                    piece(ref, src, i, o, j2, h2, sent.at[src])
                else:
                    skip = (src >= DD) & (o == 0) & (j2 == 0) & (h2 < first_heads)
                    pl.when(jnp.logical_not(skip))(lambda: piece(ref, src, i, o, j2, h2, sent.at[src]))

    def upward(o2):
        pl.semaphore_wait(ready.at[o2], 1)
        zsend(o2)

    def own_scatter():
        above = (inner - j) * (heads - head) - 1
        pl.when(above > 0)(lambda: pl.semaphore_wait(near.at[0], above))
        for i, ref in enumerate(inputs):
            scatter(o, i, ref)

    if NEARFIRST:
        own_scatter()
        if LATE:
            loop(1, o, zsend)
        loop(o + 1, outer, upward)
    else:
        loop(o + 1, jnp.minimum(o + 2, outer), upward)
        own_scatter()
        loop(o + 2, outer, upward)

    mine_part = kvd.at[0, :, pl.ds(0, rows)]
    whole = kvd.at[0, :, pl.ds(0, block)]
    part = kvd.at[0, :, pl.ds(0, (heads - 1) * rows)]

    def landed(src, dj):
        ref = whole if dj else part
        pltpu.make_async_copy(ref, ref, recv.at[src, lane(dj)]).wait()

    def arrived(src, i):
        pltpu.make_async_copy(kz.at[0, i], kz.at[0, i], zrecv.at[src, i]).wait()

    def keep(src):
        for i in range(2):
            kvd[src, i, place] = kz[src, i, :, columns(head)]

    def relay(src):
        for i in range(2):
            arrived(src, i)
            scatter(src, i, kz.at[src, i])
        keep(src)

    def relay_pair(near_one, far_one):
        def plain():
            relay(near_one)
            relay(far_one)

        def ranked():
            arrived(near_one, 0)
            scatter(near_one, 0, kz.at[near_one, 0])
            late = [(near_one, 1), (far_one, 0), (far_one, 1)]
            for src, i in late:
                arrived(src, i)
                scatter(src, i, kz.at[src, i], 0, first_heads)
            for src, i in late:
                scatter(src, i, kz.at[src, i], first_heads)
            keep(near_one)
            keep(far_one)

        if PRIO:
            pl.when(o == 0)(ranked)
            pl.when(o > 0)(plain)
        else:
            plain()

    half = max(outer // 2, 1)
    turned = jnp.minimum(o // half, 1)
    seen_from = o + turned * (outer - 1 - 2 * o)

    def source(i):
        a = i + (i + outer - seen_from) // outer
        return a + turned * (outer - 1 - 2 * a)

    lanes = block

    def absorb(blocks, first=False):
        mine = order[seq]
        spots_of = [order[src * inner + l] for src, l in blocks]
        height = len(blocks) * block
        if first:
            row = lax.broadcasted_iota(jnp.int32, (height, lanes), 0)
            col = lax.broadcasted_iota(jnp.int32, (height, lanes), 1)
            start = jnp.full((height, lanes), spots_of[0], jnp.int32) * block
            for l in range(1, len(blocks)):
                start = jnp.where(row >= l * block, (spots_of[l] - l) * block, start)
            mask = mine * block + lax.rem(col, block) >= start + row
        else:
            mask = [jnp.full((1, lanes), spot, jnp.int32) < mine for spot in spots_of]

        def stack(i):
            return jnp.concatenate(
                [kvd[src, i, pl.ds(pl.multiple_of(l * block, block), block)] for src, l in blocks]
            )

        key, value = stack(0), stack(1)
        for g in range(q_heads):
            at = slice(g * block, (g + 1) * block)
            old = None if first else (high[:, at], total[:, at], acc[:, at])
            high[:, at], total[:, at], acc[:, at] = attend(
                q_ref[:, g * HD : (g + 1) * HD], key, value, mask, old
            )

    def both(src):
        for dj in range(inner):
            landed(src, dj)
        return [(src, l) for l in range(inner)]

    qload.wait()
    oload.wait()
    pltpu.make_async_copy(mine_part, mine_part, load_sem.at[0]).wait()
    relayed = outer - 1 if outer <= 8 else 0
    for i in range(relayed - 2):
        relay(source(i))
    if relayed:
        relay_pair(source(relayed - 2), source(relayed - 1))
    absorb(both(o), True)

    def further(i):
        src = source(i)
        if not relayed:
            relay(src)
        absorb(both(src))

    if relayed:
        for i in range(outer - 3):
            further(i)
    else:
        loop(0, outer - 3, further)
    ends = [source(i) for i in range(outer - 3, outer - 1)]
    if not relayed:
        for src in ends:
            relay(src)
    for src in ends:
        landed(src, 0)
    absorb([(src, j) for src in ends])
    for src in ends:
        landed(src, 1)
    absorb([(src, lane(1)) for src in ends])

    def drained(ref, sem):
        pltpu.make_async_copy(ref, ref, sem).wait()

    def pieces(n):
        return kvd.at[0, :, pl.ds(0, n * rows)]

    def drain(src):
        fewer = (src >= DD) & (o == 0)
        if DD < outer:
            for inside in range(2):
                left = spots - 1 - (first_heads - inside)
                pl.when(fewer & (corner == (inside == 1)))(lambda: drained(pieces(left), sent.at[src]))
            pl.when(jnp.logical_not(fewer))(lambda: drained(pieces(spots - 1), sent.at[src]))
        else:
            drained(pieces(spots - 1), sent.at[src])

    if outer > 1:
        drained(kz.at[pl.ds(0, outer - 1)], zsent.at[0])
    if DD < outer:
        pl.when((o >= DD) & jnp.logical_not(corner))(lambda: drained(pieces(first_heads), dsent.at[0]))
        if first_heads > 1:
            pl.when((o >= DD) & corner)(lambda: drained(pieces(first_heads - 1), dsent.at[0]))
    loop(0, outer, drain)


def finish(acc, total, out_ref):
    block, q_cols = out_ref.shape
    for g in range(q_cols // HD):
        lane = slice(g * block, (g + 1) * block)
        part = acc[:, lane] / total[:, lane]
        out_ref[:, g * HD : (g + 1) * HD] = part.T.astype(out_ref.dtype)


def local(devices, heads, queries, keys, values, block_order):
    inner = 2 if devices % 2 == 0 else 1
    outer = devices // inner
    rows, cols = keys.shape
    block, q_cols = queries.shape
    width = cols // heads
    assert width == HD and rows * heads == block
    bf16, f32 = jnp.bfloat16, jnp.float32
    lanes = q_cols // HD * block
    assert inner == 2 and outer >= 3
    acc, total = pl.pallas_call(
        functools.partial(kernel, outer, inner, heads),
        out_shape=(
            pltpu.VMEM((HD, lanes), f32),
            pltpu.VMEM((1, lanes), f32),
        ),
        in_specs=[pl.BlockSpec(memory_space=pltpu.HBM)] * 4,
        out_specs=[pl.BlockSpec(memory_space=pltpu.VMEM)] * 2,
        scratch_shapes=[
            pltpu.SMEM(block_order.shape, jnp.int32),
            pltpu.VMEM((block, q_cols), bf16),
            pltpu.VMEM((outer, 2, rows, cols), bf16),
            pltpu.VMEM((outer, 2, inner * block, width), bf16),
            pltpu.VMEM((1, lanes), f32),
            pltpu.SemaphoreType.DMA((3,)),
            pltpu.SemaphoreType.REGULAR((outer,)),
            pltpu.SemaphoreType.REGULAR((1,)),
            pltpu.SemaphoreType.DMA((1,)),
            pltpu.SemaphoreType.DMA((outer, 2)),
            pltpu.SemaphoreType.DMA((1,)),
            pltpu.SemaphoreType.DMA((outer,)),
            pltpu.SemaphoreType.DMA((outer, inner)),
        ],
        compiler_params=pltpu.CompilerParams(
            collective_id=0, has_side_effects=True, vmem_limit_bytes=67043328 - KB * 1024
        ),
    )(block_order, queries, keys, values)
    return pl.pallas_call(
        finish,
        out_shape=jax.ShapeDtypeStruct((block, q_cols), queries.dtype),
        in_specs=[pl.BlockSpec(memory_space=pltpu.VMEM)] * 2,
        out_specs=pl.BlockSpec(memory_space=pltpu.VMEM),
        compiler_params=pltpu.CompilerParams(vmem_limit_bytes=8 * 1024 * 1024),
    )(acc, total)


def solution(mesh):
    placed = (P("seq", "head"), P(("seq", "head"), None), P(("seq", "head"), None), P())
    return jax.shard_map(
        functools.partial(local, mesh.shape["seq"], mesh.shape["head"]),
        mesh=mesh, in_specs=placed, out_specs=P("seq", "head"), check_vma=False,
    )
```

```python
import functools
import math

import jax
import jax.numpy as jnp
from jax import lax
from jax.experimental import pallas as pl
from jax.experimental.pallas import tpu as pltpu
from jax.sharding import PartitionSpec as P

HD = 128
NEG = -1e30
MESH = pl.DeviceIdType.MESH
PRIO=True
SPLITZ=True
FIN=2
LATE=True
KB=600
NEARFIRST=True


FACTOR = math.log2(math.e) / math.sqrt(HD)


def attend(q, key, value, mask, old):
    s = lax.dot_general(key, q, (((1,), (1,)), ((), ())), preferred_element_type=jnp.float32)
    s = s * FACTOR
    if old is None:
        s = jnp.where(mask, s, NEG)
        top = jnp.max(s, axis=0, keepdims=True)
        p = jnp.exp2(s - top)
    else:
        block = s.shape[0] // len(mask)
        parts = [s[n * block : (n + 1) * block] for n in range(len(mask))]
        top = old[0]
        for part, shown in zip(parts, mask):
            top = jnp.where(shown, jnp.maximum(top, jnp.max(part, axis=0, keepdims=True)), top)
        p = jnp.concatenate(
            [jnp.exp2(part - jnp.where(shown, top, -NEG)) for part, shown in zip(parts, mask)]
        )
    t = jnp.sum(p, axis=0, keepdims=True)
    pv = lax.dot_general(
        value, p.astype(jnp.bfloat16), (((0,), (0,)), ((), ())), preferred_element_type=jnp.float32
    )
    if old is None:
        return top, t, pv
    scale = jnp.exp2(old[0] - top)
    return top, old[1] * scale + t, old[2] * scale + pv


def kernel(
    outer, inner, heads,
    order_hbm, q_hbm, k_hbm, v_hbm, acc, total,
    order, q_ref, kz, kvd, high,
    load_sem, ready, near, zsent, zrecv, dsent, sent, recv,
):
    rows, cols = k_hbm.shape
    block = q_ref.shape[0]
    width = kvd.shape[-1]
    q_heads = q_ref.shape[1] // HD
    seq, head = lax.axis_index("seq"), lax.axis_index("head")
    o, j = seq // inner, lax.rem(seq, inner)
    first_heads = max(heads // 2, 1)
    spots = inner * heads
    partner = o + 1 - 2 * lax.rem(o, 2)
    place = pl.ds(pl.multiple_of(j * block + head * rows, rows), rows)
    inputs = (k_hbm, v_hbm)

    def loop(first, last, body):
        lax.fori_loop(first, last, lambda k, c: (body(k), c)[1], 0)

    def columns(h):
        return pl.ds(pl.multiple_of(h * width, width), width)

    def lane(dj):
        return lax.rem(j + dj, inner)

    def signal(sem, o2, j2, h2):
        pl.semaphore_signal(sem, inc=1, device_id=(o2 * inner + j2, h2), device_id_type=MESH)

    barrier = pltpu.get_barrier_semaphore()

    def each_spot(js, hs, sem):
        def row(j2):
            def one(h2):
                pl.when((j2 != j) | (h2 != head))(lambda: signal(sem, o, j2, h2))
            loop(*hs, one)
        loop(*js, row)

    loop(o + 1, outer, lambda o2: signal(barrier, o2, j, head))
    each_spot((j, inner), (head, heads), barrier)

    own = [
        pltpu.make_async_copy(src.at[:, columns(head)], kvd.at[o, i, place], load_sem.at[0])
        for i, src in enumerate(inputs)
    ]
    qload = pltpu.make_async_copy(q_hbm, q_ref, load_sem.at[1])
    oload = pltpu.make_async_copy(order_hbm, order, load_sem.at[2])
    for c in own + [qload, oload]:
        c.start()

    ahead = o + (j + 1) * (head + 1) - 1
    pl.when(ahead > 0)(lambda: pl.semaphore_wait(barrier, ahead))

    halves = 2 if SPLITZ else 1
    per_half = heads // halves

    def zpart(f):
        return pl.ds(f * per_half * width, per_half * width)

    def zsend(o2):
        for f in range(halves):
            for i, src in enumerate(inputs):
                pltpu.make_async_remote_copy(
                    src_ref=src.at[:, zpart(f)],
                    dst_ref=kz.at[o, i, :, zpart(f)],
                    send_sem=zsent.at[0],
                    recv_sem=zrecv.at[o, f, i],
                    device_id=(o2 * inner + j, head),
                    device_id_type=MESH,
                ).start()

    loop(0, o, lambda o2: signal(ready.at[o], o2, j, head))

    def piece(ref, src, i, o2, j2, h2, sem):
        pltpu.make_async_remote_copy(
            src_ref=ref.at[:, columns(h2)],
            dst_ref=kvd.at[src, i, place],
            send_sem=sem,
            recv_sem=recv.at[src, j],
            device_id=(o2 * inner + j2, h2),
            device_id_type=MESH,
        ).start()

    if LATE:
        loop(0, jnp.minimum(o, 1), zsend)
    else:
        loop(0, o, zsend)
    each_spot((0, j + 1), (0, head + 1), near.at[0])

    def scatter(src, i, ref, targets):
        for j2, h2 in targets:
            go = ((j2 != j) | (h2 != head)) & ((j2 == j) | (src != partner))
            pl.when(go)(lambda: piece(ref, src, i, o, j2, h2, sent.at[0]))

    def places(f, lanes_of=tuple(range(inner))):
        return [(j2, h2) for j2 in lanes_of for h2 in range(f * per_half, (f + 1) * per_half)]

    every = [(j2, h2) for j2 in range(inner) for h2 in range(heads)]

    def upward(o2):
        pl.semaphore_wait(ready.at[o2], 1)
        zsend(o2)

    def own_scatter():
        above = (inner - j) * (heads - head) - 1
        pl.when(above > 0)(lambda: pl.semaphore_wait(near.at[0], above))
        for i, ref in enumerate(inputs):
            scatter(o, i, ref, every)

    if NEARFIRST:
        own_scatter()
        if LATE:
            loop(1, o, zsend)
        loop(o + 1, outer, upward)
    else:
        loop(o + 1, jnp.minimum(o + 2, outer), upward)
        own_scatter()
        loop(o + 2, outer, upward)

    mine_part = kvd.at[0, :, pl.ds(0, rows)]
    whole = kvd.at[0, :, pl.ds(0, block)]
    part = kvd.at[0, :, pl.ds(0, (heads - 1) * rows)]

    def landed(src, dj):
        ref = whole if dj else part
        pltpu.make_async_copy(ref, ref, recv.at[src, lane(dj)]).wait()

    def arrived(src, f, i):
        ref = kz.at[0, i, :, zpart(f)]
        pltpu.make_async_copy(ref, ref, zrecv.at[src, f, i]).wait()

    def keep(src):
        for i in range(2):
            kvd[src, i, place] = kz[src, i, :, columns(head)]

    def relay(src, parts=tuple(range(2 if SPLITZ else 1))):
        for f in parts:
            for i in range(2):
                arrived(src, f, i)
                scatter(src, i, kz.at[src, i], places(f))

    def relay_pair(*srcs):
        def plain():
            for src in srcs:
                relay(src)

        def ranked():
            late = [(src, i) for src in srcs for i in range(2)]
            for src, i in late:
                arrived(src, 0, i)
                scatter(src, i, kz.at[src, i], places(0, (0,)))
            for src, i in late:
                scatter(src, i, kz.at[src, i], places(0, tuple(range(1, inner))))
            for src in srcs:
                relay(src, tuple(range(1, halves)))

        if PRIO:
            pl.when(o == 0)(ranked)
            pl.when(o > 0)(plain)
        else:
            plain()
        for src in srcs:
            keep(src)

    half = max(outer // 2, 1)
    turned = jnp.minimum(o // half, 1)
    seen_from = o + turned * (outer - 1 - 2 * o)

    def source(i):
        a = i + (i + outer - seen_from) // outer
        return a + turned * (outer - 1 - 2 * a)

    lanes = block

    def absorb(blocks, first=False):
        mine = order[seq]
        spots_of = [order[src * inner + l] for src, l in blocks]
        height = len(blocks) * block
        if first:
            row = lax.broadcasted_iota(jnp.int32, (height, lanes), 0)
            col = lax.broadcasted_iota(jnp.int32, (height, lanes), 1)
            start = jnp.full((height, lanes), spots_of[0], jnp.int32) * block
            for l in range(1, len(blocks)):
                start = jnp.where(row >= l * block, (spots_of[l] - l) * block, start)
            mask = mine * block + lax.rem(col, block) >= start + row
        else:
            mask = [jnp.full((1, lanes), spot, jnp.int32) < mine for spot in spots_of]

        def stack(i):
            return jnp.concatenate(
                [kvd[src, i, pl.ds(pl.multiple_of(l * block, block), block)] for src, l in blocks]
            )

        key, value = stack(0), stack(1)
        for g in range(q_heads):
            at = slice(g * block, (g + 1) * block)
            old = None if first else (high[:, at], total[:, at], acc[:, at])
            high[:, at], total[:, at], acc[:, at] = attend(
                q_ref[:, g * HD : (g + 1) * HD], key, value, mask, old
            )

    def both(src):
        for dj in range(inner):
            landed(src, dj)
        return [(src, l) for l in range(inner)]

    qload.wait()
    oload.wait()
    pltpu.make_async_copy(mine_part, mine_part, load_sem.at[0]).wait()
    across = kvd.at[o, :, pl.ds(pl.multiple_of(lane(1) * block, block), block)]

    def hand_over():
        landed(o, 1)
        pltpu.make_async_remote_copy(
            src_ref=across,
            dst_ref=across,
            send_sem=dsent.at[0],
            recv_sem=recv.at[o, lane(1)],
            device_id=(partner * inner + j, head),
            device_id_type=MESH,
        ).start()

    relayed = outer - 1 if outer <= 8 else 0
    for i in range(relayed - 2):
        relay(source(i))
        keep(source(i))
    hand_over()
    if relayed:
        relay_pair(source(relayed - 2), source(relayed - 1))
    landed(o, 0)
    absorb([(o, l) for l in range(inner)], True)

    def further(i):
        src = source(i)
        if not relayed:
            relay(src)
            keep(src)
        absorb(both(src))

    if relayed:
        for i in range(outer - 3):
            further(i)
    else:
        loop(0, outer - 3, further)
    ends = [source(i) for i in range(outer - 3, outer - 1)]
    if not relayed:
        for src in ends:
            relay(src)
            keep(src)
    for src in ends:
        landed(src, 0)
    absorb([(src, j) for src in ends])
    for src in ends:
        landed(src, 1)
    absorb([(src, lane(1)) for src in ends])

    def drained(ref, sem):
        pltpu.make_async_copy(ref, ref, sem).wait()

    drained(kz.at[pl.ds(0, outer - 1)], zsent.at[0])
    drained(whole, dsent.at[0])
    scattered = outer * (spots - 1) - (spots - heads)
    drained(kvd.at[:, :, pl.ds(0, scattered * rows // outer)], sent.at[0])


def finish(acc, total, out_hbm, out, sem):
    block, q_cols = out.shape
    count = sem.shape[0]
    wide = q_cols // count
    copies = []
    for n in range(count):
        for g in range(n * wide // HD, (n + 1) * wide // HD):
            lane = slice(g * block, (g + 1) * block)
            part = acc[:, lane] * (1.0 / total[:, lane])
            out[:, g * HD : (g + 1) * HD] = part.astype(out.dtype).T
        at = pl.ds(n * wide, wide)
        copies.append(pltpu.make_async_copy(out.at[:, at], out_hbm.at[:, at], sem.at[n]))
        copies[-1].start()
    for copy in copies:
        copy.wait()


def local(devices, heads, queries, keys, values, block_order):
    inner = 2 if devices % 2 == 0 else 1
    outer = devices // inner
    rows, cols = keys.shape
    block, q_cols = queries.shape
    width = cols // heads
    assert width == HD and rows * heads == block
    bf16, f32 = jnp.bfloat16, jnp.float32
    lanes = q_cols // HD * block
    assert inner == 2 and outer >= 3
    acc, total = pl.pallas_call(
        functools.partial(kernel, outer, inner, heads),
        out_shape=(
            pltpu.VMEM((HD, lanes), f32),
            pltpu.VMEM((1, lanes), f32),
        ),
        in_specs=[pl.BlockSpec(memory_space=pltpu.HBM)] * 4,
        out_specs=[pl.BlockSpec(memory_space=pltpu.VMEM)] * 2,
        scratch_shapes=[
            pltpu.SMEM(block_order.shape, jnp.int32),
            pltpu.VMEM((block, q_cols), bf16),
            pltpu.VMEM((outer, 2, rows, cols), bf16),
            pltpu.VMEM((outer, 2, inner * block, width), bf16),
            pltpu.VMEM((1, lanes), f32),
            pltpu.SemaphoreType.DMA((3,)),
            pltpu.SemaphoreType.REGULAR((outer,)),
            pltpu.SemaphoreType.REGULAR((1,)),
            pltpu.SemaphoreType.DMA((1,)),
            pltpu.SemaphoreType.DMA((outer, 2 if SPLITZ else 1, 2)),
            pltpu.SemaphoreType.DMA((1,)),
            pltpu.SemaphoreType.DMA((1,)),
            pltpu.SemaphoreType.DMA((outer, inner)),
        ],
        compiler_params=pltpu.CompilerParams(
            collective_id=0, has_side_effects=True, vmem_limit_bytes=67043328 - KB * 1024
        ),
    )(block_order, queries, keys, values)
    return pl.pallas_call(
        finish,
        out_shape=jax.ShapeDtypeStruct((block, q_cols), queries.dtype),
        in_specs=[pl.BlockSpec(memory_space=pltpu.VMEM)] * 2,
        out_specs=pl.BlockSpec(memory_space=pltpu.HBM),
        scratch_shapes=[
            pltpu.VMEM((block, q_cols), queries.dtype),
            pltpu.SemaphoreType.DMA((FIN,)),
        ],
        compiler_params=pltpu.CompilerParams(vmem_limit_bytes=8 * 1024 * 1024),
    )(acc, total)


def solution(mesh):
    placed = (P("seq", "head"), P(("seq", "head"), None), P(("seq", "head"), None), P())
    return jax.shard_map(
        functools.partial(local, mesh.shape["seq"], mesh.shape["head"]),
        mesh=mesh, in_specs=placed, out_specs=P("seq", "head"), check_vma=False,
    )
```

```python
import functools
import math

import jax
import jax.numpy as jnp
from jax import lax
from jax.experimental import pallas as pl
from jax.experimental.pallas import tpu as pltpu
from jax.sharding import PartitionSpec as P

HD = 128
NEG = -1e30
MESH = pl.DeviceIdType.MESH
PRIO=True
SPLITZ=True
FIN=2
MODE=0
LATE=True
KB=600
NEARFIRST=True


FACTOR = math.log2(math.e) / math.sqrt(HD)


def attend(q, key, value, mask, old):
    s = lax.dot_general(key, q, (((1,), (1,)), ((), ())), preferred_element_type=jnp.float32)
    s = s * FACTOR
    if old is None:
        s = jnp.where(mask, s, NEG)
        top = jnp.max(s, axis=0, keepdims=True)
        p = jnp.exp2(s - top)
    else:
        block = s.shape[0] // len(mask)
        parts = [s[n * block : (n + 1) * block] for n in range(len(mask))]
        top = old[0]
        for part, shown in zip(parts, mask):
            top = jnp.where(shown, jnp.maximum(top, jnp.max(part, axis=0, keepdims=True)), top)
        p = jnp.concatenate(
            [jnp.exp2(part - jnp.where(shown, top, -NEG)) for part, shown in zip(parts, mask)]
        )
    t = jnp.sum(p, axis=0, keepdims=True)
    pv = lax.dot_general(
        value, p.astype(jnp.bfloat16), (((0,), (0,)), ((), ())), preferred_element_type=jnp.float32
    )
    if old is None:
        return top, t, pv
    scale = jnp.exp2(old[0] - top)
    return top, old[1] * scale + t, old[2] * scale + pv


def kernel(
    outer, inner, heads,
    order_hbm, q_hbm, k_hbm, v_hbm, acc, total,
    order, q_ref, kz, kvd, high,
    load_sem, ready, near, zsent, zrecv, dsent, sent, recv,
):
    rows, cols = k_hbm.shape
    block = q_ref.shape[0]
    width = kvd.shape[-1]
    q_heads = q_ref.shape[1] // HD
    seq, head = lax.axis_index("seq"), lax.axis_index("head")
    o, j = seq // inner, lax.rem(seq, inner)
    first_heads = max(heads // 2, 1)
    spots = inner * heads
    partner = o + 1 - 2 * lax.rem(o, 2)
    place = pl.ds(pl.multiple_of(j * block + head * rows, rows), rows)
    inputs = (k_hbm, v_hbm)

    def loop(first, last, body):
        lax.fori_loop(first, last, lambda k, c: (body(k), c)[1], 0)

    def columns(h):
        return pl.ds(pl.multiple_of(h * width, width), width)

    def lane(dj):
        return lax.rem(j + dj, inner)

    def signal(sem, o2, j2, h2):
        pl.semaphore_signal(sem, inc=1, device_id=(o2 * inner + j2, h2), device_id_type=MESH)

    barrier = pltpu.get_barrier_semaphore()

    def each_spot(js, hs, sem):
        def row(j2):
            def one(h2):
                pl.when((j2 != j) | (h2 != head))(lambda: signal(sem, o, j2, h2))
            loop(*hs, one)
        loop(*js, row)

    loop(o + 1, outer, lambda o2: signal(barrier, o2, j, head))
    each_spot((j, inner), (head, heads), barrier)

    own = [
        pltpu.make_async_copy(src.at[:, columns(head)], kvd.at[o, i, place], load_sem.at[0])
        for i, src in enumerate(inputs)
    ]
    qload = pltpu.make_async_copy(q_hbm, q_ref, load_sem.at[1])
    oload = pltpu.make_async_copy(order_hbm, order, load_sem.at[2])
    for c in own + [qload, oload]:
        c.start()

    ahead = o + (j + 1) * (head + 1) - 1
    pl.when(ahead > 0)(lambda: pl.semaphore_wait(barrier, ahead))

    halves = 2 if SPLITZ else 1
    per_half = heads // halves

    def zpart(f):
        return pl.ds(f * per_half * width, per_half * width)

    def zsend(o2):
        for f in range(halves):
            for i, src in enumerate(inputs):
                pltpu.make_async_remote_copy(
                    src_ref=src.at[:, zpart(f)],
                    dst_ref=kz.at[o, i, :, zpart(f)],
                    send_sem=zsent.at[0],
                    recv_sem=zrecv.at[o, f, i],
                    device_id=(o2 * inner + j, head),
                    device_id_type=MESH,
                ).start()

    loop(0, o, lambda o2: signal(ready.at[o], o2, j, head))

    def piece(ref, src, i, o2, j2, h2, sem):
        pltpu.make_async_remote_copy(
            src_ref=ref.at[:, columns(h2)],
            dst_ref=kvd.at[src, i, place],
            send_sem=sem,
            recv_sem=recv.at[src, j],
            device_id=(o2 * inner + j2, h2),
            device_id_type=MESH,
        ).start()

    if LATE:
        loop(0, jnp.minimum(o, 1), zsend)
    else:
        loop(0, o, zsend)
    each_spot((0, j + 1), (0, head + 1), near.at[0])

    def scatter(src, i, ref, targets):
        for j2, h2 in targets:
            go = ((j2 != j) | (h2 != head)) & ((j2 == j) | (src != partner))
            pl.when(go)(lambda: piece(ref, src, i, o, j2, h2, sent.at[0]))

    def places(f, lanes_of=tuple(range(inner))):
        return [(j2, h2) for j2 in lanes_of for h2 in range(f * per_half, (f + 1) * per_half)]

    every = [(j2, h2) for j2 in range(inner) for h2 in range(heads)]

    def upward(o2):
        pl.semaphore_wait(ready.at[o2], 1)
        zsend(o2)

    def own_scatter():
        above = (inner - j) * (heads - head) - 1
        pl.when(above > 0)(lambda: pl.semaphore_wait(near.at[0], above))
        for i, ref in enumerate(inputs):
            scatter(o, i, ref, every)

    if NEARFIRST:
        own_scatter()
        if LATE:
            loop(1, o, zsend)
        loop(o + 1, outer, upward)
    else:
        loop(o + 1, jnp.minimum(o + 2, outer), upward)
        own_scatter()
        loop(o + 2, outer, upward)

    mine_part = kvd.at[0, :, pl.ds(0, rows)]
    whole = kvd.at[0, :, pl.ds(0, block)]
    part = kvd.at[0, :, pl.ds(0, (heads - 1) * rows)]

    def landed(src, dj):
        ref = whole if dj else part
        pltpu.make_async_copy(ref, ref, recv.at[src, lane(dj)]).wait()

    def arrived(src, f, i):
        ref = kz.at[0, i, :, zpart(f)]
        pltpu.make_async_copy(ref, ref, zrecv.at[src, f, i]).wait()

    def keep(src):
        for i in range(2):
            kvd[src, i, place] = kz[src, i, :, columns(head)]

    def relay(src, parts=tuple(range(2 if SPLITZ else 1))):
        for f in parts:
            for i in range(2):
                arrived(src, f, i)
                scatter(src, i, kz.at[src, i], places(f))

    def relay_pair(*srcs):
        def plain():
            for src in srcs:
                relay(src)

        def ranked():
            late = [(src, i) for src in srcs for i in range(2)]
            for src, i in late:
                arrived(src, 0, i)
                scatter(src, i, kz.at[src, i], places(0, (0,)))
            for src, i in late:
                scatter(src, i, kz.at[src, i], places(0, tuple(range(1, inner))))
            for src in srcs:
                relay(src, tuple(range(1, halves)))

        if PRIO:
            pl.when(o == 0)(ranked)
            pl.when(o > 0)(plain)
        else:
            plain()
        for src in srcs:
            keep(src)

    half = max(outer // 2, 1)
    turned = jnp.minimum(o // half, 1)
    seen_from = o + turned * (outer - 1 - 2 * o)

    def source(i):
        a = i + (i + outer - seen_from) // outer
        return a + turned * (outer - 1 - 2 * a)

    lanes = block

    def absorb(blocks, first=False):
        mine = order[seq]
        spots_of = [order[src * inner + l] for src, l in blocks]
        height = len(blocks) * block
        if first:
            row = lax.broadcasted_iota(jnp.int32, (height, lanes), 0)
            col = lax.broadcasted_iota(jnp.int32, (height, lanes), 1)
            start = jnp.full((height, lanes), spots_of[0], jnp.int32) * block
            for l in range(1, len(blocks)):
                start = jnp.where(row >= l * block, (spots_of[l] - l) * block, start)
            mask = mine * block + lax.rem(col, block) >= start + row
        else:
            mask = [jnp.full((1, lanes), spot, jnp.int32) < mine for spot in spots_of]

        def stack(i):
            return jnp.concatenate(
                [kvd[src, i, pl.ds(pl.multiple_of(l * block, block), block)] for src, l in blocks]
            )

        key, value = stack(0), stack(1)
        for g in range(q_heads):
            at = slice(g * block, (g + 1) * block)
            old = None if first else (high[:, at], total[:, at], acc[:, at])
            high[:, at], total[:, at], acc[:, at] = attend(
                q_ref[:, g * HD : (g + 1) * HD], key, value, mask, old
            )

    def both(src):
        for dj in range(inner):
            landed(src, dj)
        return [(src, l) for l in range(inner)]

    qload.wait()
    oload.wait()
    pltpu.make_async_copy(mine_part, mine_part, load_sem.at[0]).wait()
    across = kvd.at[o, :, pl.ds(pl.multiple_of(lane(1) * block, block), block)]

    def hand_over():
        landed(o, 1)
        pltpu.make_async_remote_copy(
            src_ref=across,
            dst_ref=across,
            send_sem=dsent.at[0],
            recv_sem=recv.at[o, lane(1)],
            device_id=(partner * inner + j, head),
            device_id_type=MESH,
        ).start()

    relayed = outer - 1 if outer <= 8 else 0
    for i in range(relayed - 2):
        relay(source(i))
        keep(source(i))
    hand_over()
    if relayed:
        relay_pair(source(relayed - 2), source(relayed - 1))
    landed(o, 0)
    absorb([(o, l) for l in range(inner)], True)

    def further(i):
        src = source(i)
        if not relayed:
            relay(src)
            keep(src)
        absorb(both(src))

    if relayed:
        for i in range(outer - 3):
            further(i)
    else:
        loop(0, outer - 3, further)
    ends = [source(i) for i in range(outer - 3, outer - 1)]
    if not relayed:
        for src in ends:
            relay(src)
            keep(src)
    front = 1 - jnp.minimum(o, 1)
    if MODE == 1:
        front = front * 0
    if MODE == 2:
        front = front * 0 + 1
    near_one, far_one = ends
    landed(near_one, 0)
    pl.when(front == 1)(lambda: landed(far_one, 0))
    pl.when(front == 0)(lambda: landed(near_one, 1))
    turn = front * (far_one - near_one)
    absorb([(near_one, j), (near_one + turn, lane(1) + front * (j - lane(1)))])
    pl.when(front == 1)(lambda: landed(near_one, 1))
    pl.when(front == 0)(lambda: landed(far_one, 0))
    landed(far_one, 1)
    absorb([(far_one - turn, j + front * (lane(1) - j)), (far_one, lane(1))])

    def drained(ref, sem):
        pltpu.make_async_copy(ref, ref, sem).wait()

    drained(kz.at[pl.ds(0, outer - 1)], zsent.at[0])
    drained(whole, dsent.at[0])
    scattered = outer * (spots - 1) - (spots - heads)
    drained(kvd.at[:, :, pl.ds(0, scattered * rows // outer)], sent.at[0])


def finish(acc, total, out_hbm, out, sem):
    block, q_cols = out.shape
    count = sem.shape[0]
    wide = q_cols // count
    copies = []
    for n in range(count):
        for g in range(n * wide // HD, (n + 1) * wide // HD):
            lane = slice(g * block, (g + 1) * block)
            part = acc[:, lane] * (1.0 / total[:, lane])
            out[:, g * HD : (g + 1) * HD] = part.astype(out.dtype).T
        at = pl.ds(n * wide, wide)
        copies.append(pltpu.make_async_copy(out.at[:, at], out_hbm.at[:, at], sem.at[n]))
        copies[-1].start()
    for copy in copies:
        copy.wait()


def local(devices, heads, queries, keys, values, block_order):
    inner = 2 if devices % 2 == 0 else 1
    outer = devices // inner
    rows, cols = keys.shape
    block, q_cols = queries.shape
    width = cols // heads
    assert width == HD and rows * heads == block
    bf16, f32 = jnp.bfloat16, jnp.float32
    lanes = q_cols // HD * block
    assert inner == 2 and outer >= 3
    acc, total = pl.pallas_call(
        functools.partial(kernel, outer, inner, heads),
        out_shape=(
            pltpu.VMEM((HD, lanes), f32),
            pltpu.VMEM((1, lanes), f32),
        ),
        in_specs=[pl.BlockSpec(memory_space=pltpu.HBM)] * 4,
        out_specs=[pl.BlockSpec(memory_space=pltpu.VMEM)] * 2,
        scratch_shapes=[
            pltpu.SMEM(block_order.shape, jnp.int32),
            pltpu.VMEM((block, q_cols), bf16),
            pltpu.VMEM((outer, 2, rows, cols), bf16),
            pltpu.VMEM((outer, 2, inner * block, width), bf16),
            pltpu.VMEM((1, lanes), f32),
            pltpu.SemaphoreType.DMA((3,)),
            pltpu.SemaphoreType.REGULAR((outer,)),
            pltpu.SemaphoreType.REGULAR((1,)),
            pltpu.SemaphoreType.DMA((1,)),
            pltpu.SemaphoreType.DMA((outer, 2 if SPLITZ else 1, 2)),
            pltpu.SemaphoreType.DMA((1,)),
            pltpu.SemaphoreType.DMA((1,)),
            pltpu.SemaphoreType.DMA((outer, inner)),
        ],
        compiler_params=pltpu.CompilerParams(
            collective_id=0, has_side_effects=True, vmem_limit_bytes=67043328 - KB * 1024
        ),
    )(block_order, queries, keys, values)
    return pl.pallas_call(
        finish,
        out_shape=jax.ShapeDtypeStruct((block, q_cols), queries.dtype),
        in_specs=[pl.BlockSpec(memory_space=pltpu.VMEM)] * 2,
        out_specs=pl.BlockSpec(memory_space=pltpu.HBM),
        scratch_shapes=[
            pltpu.VMEM((block, q_cols), queries.dtype),
            pltpu.SemaphoreType.DMA((FIN,)),
        ],
        compiler_params=pltpu.CompilerParams(vmem_limit_bytes=8 * 1024 * 1024),
    )(acc, total)


def solution(mesh):
    placed = (P("seq", "head"), P(("seq", "head"), None), P(("seq", "head"), None), P())
    return jax.shard_map(
        functools.partial(local, mesh.shape["seq"], mesh.shape["head"]),
        mesh=mesh, in_specs=placed, out_specs=P("seq", "head"), check_vma=False,
    )
```

```python
import functools
import math

import jax
import jax.numpy as jnp
from jax import lax
from jax.experimental import pallas as pl
from jax.experimental.pallas import tpu as pltpu
from jax.sharding import PartitionSpec as P

HD = 128
NEG = -1e30
MESH = pl.DeviceIdType.MESH
HALVES = 2
CHUNKS = 2


FACTOR = math.log2(math.e) / math.sqrt(HD)


def attend(q, key, value, mask, old):
    s = lax.dot_general(key, q, (((1,), (1,)), ((), ())), preferred_element_type=jnp.float32)
    s = s * FACTOR
    if old is None:
        s = jnp.where(mask, s, NEG)
        top = jnp.max(s, axis=0, keepdims=True)
        p = jnp.exp2(s - top)
    else:
        block = s.shape[0] // len(mask)
        parts = [s[n * block : (n + 1) * block] for n in range(len(mask))]
        top = old[0]
        for part, shown in zip(parts, mask):
            top = jnp.where(shown, jnp.maximum(top, jnp.max(part, axis=0, keepdims=True)), top)
        p = jnp.concatenate(
            [jnp.exp2(part - jnp.where(shown, top, -NEG)) for part, shown in zip(parts, mask)]
        )
    t = jnp.sum(p, axis=0, keepdims=True)
    pv = lax.dot_general(
        value, p.astype(jnp.bfloat16), (((0,), (0,)), ((), ())), preferred_element_type=jnp.float32
    )
    if old is None:
        return top, t, pv
    scale = jnp.exp2(old[0] - top)
    return top, old[1] * scale + t, old[2] * scale + pv


def kernel(
    outer, inner, heads,
    order_hbm, q_hbm, k_hbm, v_hbm, acc, total,
    order, q_ref, kz, kvd, high,
    load_sem, ready, near, zsent, zrecv, sent, recv,
):
    rows, cols = k_hbm.shape
    block = q_ref.shape[0]
    width = kvd.shape[-1]
    q_heads = q_ref.shape[1] // HD
    seq, head = lax.axis_index("seq"), lax.axis_index("head")
    o, j = seq // inner, lax.rem(seq, inner)
    first_heads = max(heads // 2, 1)
    spots = inner * heads
    place = pl.ds(pl.multiple_of(j * block + head * rows, rows), rows)
    inputs = (k_hbm, v_hbm)

    def loop(first, last, body):
        lax.fori_loop(first, last, lambda k, c: (body(k), c)[1], 0)

    def columns(h):
        return pl.ds(pl.multiple_of(h * width, width), width)

    def lane(dj):
        return lax.rem(j + dj, inner)

    def signal(sem, o2, j2, h2):
        pl.semaphore_signal(sem, inc=1, device_id=(o2 * inner + j2, h2), device_id_type=MESH)

    barrier = pltpu.get_barrier_semaphore()

    def each_spot(js, hs, sem):
        def row(j2):
            def one(h2):
                pl.when((j2 != j) | (h2 != head))(lambda: signal(sem, o, j2, h2))
            loop(*hs, one)
        loop(*js, row)

    loop(o + 1, outer, lambda o2: signal(barrier, o2, j, head))
    each_spot((j, inner), (head, heads), barrier)

    own = [
        pltpu.make_async_copy(src.at[:, columns(head)], kvd.at[o, i, place], load_sem.at[0])
        for i, src in enumerate(inputs)
    ]
    qload = pltpu.make_async_copy(q_hbm, q_ref, load_sem.at[1])
    oload = pltpu.make_async_copy(order_hbm, order, load_sem.at[2])
    for c in own + [qload, oload]:
        c.start()

    ahead = o + (j + 1) * (head + 1) - 1
    pl.when(ahead > 0)(lambda: pl.semaphore_wait(barrier, ahead))

    halves = HALVES
    per_half = heads // halves

    def zpart(f):
        return pl.ds(f * per_half * width, per_half * width)

    def zsend(o2):
        for f in range(halves):
            for i, src in enumerate(inputs):
                pltpu.make_async_remote_copy(
                    src_ref=src.at[:, zpart(f)],
                    dst_ref=kz.at[o, i, :, zpart(f)],
                    send_sem=zsent.at[0],
                    recv_sem=zrecv.at[o, f, i],
                    device_id=(o2 * inner + j, head),
                    device_id_type=MESH,
                ).start()

    loop(0, o, lambda o2: signal(ready.at[o], o2, j, head))

    def piece(ref, src, i, o2, j2, h2, sem):
        pltpu.make_async_remote_copy(
            src_ref=ref.at[:, columns(h2)],
            dst_ref=kvd.at[src, i, place],
            send_sem=sem,
            recv_sem=recv.at[src, j],
            device_id=(o2 * inner + j2, h2),
            device_id_type=MESH,
        ).start()

    loop(0, jnp.minimum(o, 1), zsend)
    each_spot((0, j + 1), (0, head + 1), near.at[0])

    def scatter(src, i, ref, targets):
        for j2, h2 in targets:
            go = (j2 != j) | (h2 != head)
            pl.when(go)(lambda: piece(ref, src, i, o, j2, h2, sent.at[0]))

    def places(f, lanes_of=tuple(range(inner))):
        return [(j2, h2) for j2 in lanes_of for h2 in range(f * per_half, (f + 1) * per_half)]

    every = [(j2, h2) for j2 in range(inner) for h2 in range(heads)]

    def upward(o2):
        pl.semaphore_wait(ready.at[o2], 1)
        zsend(o2)

    def own_scatter():
        above = (inner - j) * (heads - head) - 1
        pl.when(above > 0)(lambda: pl.semaphore_wait(near.at[0], above))
        for i, ref in enumerate(inputs):
            scatter(o, i, ref, every)

    loop(1, o, zsend)
    own_scatter()
    loop(o + 1, outer, upward)

    mine_part = kvd.at[0, :, pl.ds(0, rows)]
    whole = kvd.at[0, :, pl.ds(0, block)]
    part = kvd.at[0, :, pl.ds(0, (heads - 1) * rows)]

    def landed(src, dj):
        ref = whole if dj else part
        pltpu.make_async_copy(ref, ref, recv.at[src, lane(dj)]).wait()

    def arrived(src, f, i):
        ref = kz.at[0, i, :, zpart(f)]
        pltpu.make_async_copy(ref, ref, zrecv.at[src, f, i]).wait()

    def keep(src):
        for i in range(2):
            kvd[src, i, place] = kz[src, i, :, columns(head)]

    def relay(src, parts=tuple(range(HALVES))):
        for f in parts:
            for i in range(2):
                arrived(src, f, i)
                scatter(src, i, kz.at[src, i], places(f))

    def relay_pair(*srcs):
        late = [(src, i) for src in srcs for i in range(2)]
        for src, i in late:
            arrived(src, 0, i)
            scatter(src, i, kz.at[src, i], places(0, (0,)))
        for src, i in late:
            scatter(src, i, kz.at[src, i], places(0, tuple(range(1, inner))))
        for src in srcs:
            relay(src, tuple(range(1, halves)))
        for src in srcs:
            keep(src)

    half = max(outer // 2, 1)
    turned = jnp.minimum(o // half, 1)
    seen_from = o + turned * (outer - 1 - 2 * o)

    def source(i):
        a = i + (i + outer - seen_from) // outer
        return a + turned * (outer - 1 - 2 * a)

    lanes = block

    def absorb(blocks, first=False):
        mine = order[seq]
        spots_of = [order[src * inner + l] for src, l in blocks]
        height = len(blocks) * block
        if first:
            row = lax.broadcasted_iota(jnp.int32, (height, lanes), 0)
            col = lax.broadcasted_iota(jnp.int32, (height, lanes), 1)
            start = jnp.full((height, lanes), spots_of[0], jnp.int32) * block
            for l in range(1, len(blocks)):
                start = jnp.where(row >= l * block, (spots_of[l] - l) * block, start)
            mask = mine * block + lax.rem(col, block) >= start + row
        else:
            mask = [jnp.full((1, lanes), spot, jnp.int32) < mine for spot in spots_of]

        def stack(i):
            return jnp.concatenate(
                [kvd[src, i, pl.ds(pl.multiple_of(l * block, block), block)] for src, l in blocks]
            )

        key, value = stack(0), stack(1)
        for g in range(q_heads):
            at = slice(g * block, (g + 1) * block)
            old = None if first else (high[:, at], total[:, at], acc[:, at])
            high[:, at], total[:, at], acc[:, at] = attend(
                q_ref[:, g * HD : (g + 1) * HD], key, value, mask, old
            )

    def both(src):
        for dj in range(inner):
            landed(src, dj)
        return [(src, l) for l in range(inner)]

    qload.wait()
    oload.wait()
    pltpu.make_async_copy(mine_part, mine_part, load_sem.at[0]).wait()
    relayed = outer - 1 if outer <= 8 else 0
    for i in range(relayed - 2):
        relay(source(i))
        keep(source(i))
    if relayed:
        relay_pair(source(relayed - 2), source(relayed - 1))
    absorb(both(o), True)

    def further(i):
        src = source(i)
        if not relayed:
            relay(src)
            keep(src)
        absorb(both(src))

    if relayed:
        for i in range(outer - 3):
            further(i)
    else:
        loop(0, outer - 3, further)
    ends = [source(i) for i in range(outer - 3, outer - 1)]
    if not relayed:
        for src in ends:
            relay(src)
            keep(src)
    front = 1 - jnp.minimum(o, 1)
    near_one, far_one = ends
    landed(near_one, 0)
    pl.when(front == 1)(lambda: landed(far_one, 0))
    pl.when(front == 0)(lambda: landed(near_one, 1))
    turn = front * (far_one - near_one)
    absorb([(near_one, j), (near_one + turn, lane(1) + front * (j - lane(1)))])
    pl.when(front == 1)(lambda: landed(near_one, 1))
    pl.when(front == 0)(lambda: landed(far_one, 0))
    landed(far_one, 1)
    absorb([(far_one - turn, j + front * (lane(1) - j)), (far_one, lane(1))])

    def drained(ref, sem):
        pltpu.make_async_copy(ref, ref, sem).wait()

    drained(kz.at[pl.ds(0, outer - 1)], zsent.at[0])
    scattered = outer * (spots - 1)
    drained(kvd.at[:, :, pl.ds(0, scattered * rows // outer)], sent.at[0])


def finish(acc, total, out_hbm, out, sem):
    block, q_cols = out.shape
    count = sem.shape[0]
    wide = q_cols // count
    copies = []
    for n in range(count):
        for g in range(n * wide // HD, (n + 1) * wide // HD):
            lane = slice(g * block, (g + 1) * block)
            part = acc[:, lane] * (1.0 / total[:, lane])
            out[:, g * HD : (g + 1) * HD] = part.astype(out.dtype).T
        at = pl.ds(n * wide, wide)
        copies.append(pltpu.make_async_copy(out.at[:, at], out_hbm.at[:, at], sem.at[n]))
        copies[-1].start()
    for copy in copies:
        copy.wait()


def local(devices, heads, queries, keys, values, block_order):
    inner = 2 if devices % 2 == 0 else 1
    outer = devices // inner
    rows, cols = keys.shape
    block, q_cols = queries.shape
    width = cols // heads
    assert width == HD and rows * heads == block
    bf16, f32 = jnp.bfloat16, jnp.float32
    lanes = q_cols // HD * block
    assert inner == 2 and outer >= 3
    acc, total = pl.pallas_call(
        functools.partial(kernel, outer, inner, heads),
        out_shape=(
            pltpu.VMEM((HD, lanes), f32),
            pltpu.VMEM((1, lanes), f32),
        ),
        in_specs=[pl.BlockSpec(memory_space=pltpu.HBM)] * 4,
        out_specs=[pl.BlockSpec(memory_space=pltpu.VMEM)] * 2,
        scratch_shapes=[
            pltpu.SMEM(block_order.shape, jnp.int32),
            pltpu.VMEM((block, q_cols), bf16),
            pltpu.VMEM((outer, 2, rows, cols), bf16),
            pltpu.VMEM((outer, 2, inner * block, width), bf16),
            pltpu.VMEM((1, lanes), f32),
            pltpu.SemaphoreType.DMA((3,)),
            pltpu.SemaphoreType.REGULAR((outer,)),
            pltpu.SemaphoreType.REGULAR((1,)),
            pltpu.SemaphoreType.DMA((1,)),
            pltpu.SemaphoreType.DMA((outer, HALVES, 2)),
            pltpu.SemaphoreType.DMA((1,)),
            pltpu.SemaphoreType.DMA((outer, inner)),
        ],
        compiler_params=pltpu.CompilerParams(
            collective_id=0, has_side_effects=True, vmem_limit_bytes=67043328 - 600 * 1024
        ),
    )(block_order, queries, keys, values)
    return pl.pallas_call(
        finish,
        out_shape=jax.ShapeDtypeStruct((block, q_cols), queries.dtype),
        in_specs=[pl.BlockSpec(memory_space=pltpu.VMEM)] * 2,
        out_specs=pl.BlockSpec(memory_space=pltpu.HBM),
        scratch_shapes=[
            pltpu.VMEM((block, q_cols), queries.dtype),
            pltpu.SemaphoreType.DMA((CHUNKS,)),
        ],
        compiler_params=pltpu.CompilerParams(vmem_limit_bytes=8 * 1024 * 1024),
    )(acc, total)


def solution(mesh):
    placed = (P("seq", "head"), P(("seq", "head"), None), P(("seq", "head"), None), P())
    return jax.shard_map(
        functools.partial(local, mesh.shape["seq"], mesh.shape["head"]),
        mesh=mesh, in_specs=placed, out_specs=P("seq", "head"), check_vma=False,
    )
```

```python
import functools
import math

import jax
import jax.numpy as jnp
from jax import lax
from jax.experimental import pallas as pl
from jax.experimental.pallas import tpu as pltpu
from jax.sharding import PartitionSpec as P

HD = 128
NEG = -1e30
MESH = pl.DeviceIdType.MESH
CHUNKS = 2


FACTOR = math.log2(math.e) / math.sqrt(HD)


def attend(q, key, value, mask, old):
    s = lax.dot_general(key, q, (((1,), (1,)), ((), ())), preferred_element_type=jnp.float32)
    s = s * FACTOR
    if old is None:
        s = jnp.where(mask, s, NEG)
        top = jnp.max(s, axis=0, keepdims=True)
        p = jnp.exp2(s - top)
    else:
        block = s.shape[0] // len(mask)
        parts = [s[n * block : (n + 1) * block] for n in range(len(mask))]
        top = old[0]
        for part, shown in zip(parts, mask):
            top = jnp.where(shown, jnp.maximum(top, jnp.max(part, axis=0, keepdims=True)), top)
        p = jnp.concatenate(
            [jnp.exp2(part - jnp.where(shown, top, -NEG)) for part, shown in zip(parts, mask)]
        )
    t = jnp.sum(p, axis=0, keepdims=True)
    pv = lax.dot_general(
        value, p.astype(jnp.bfloat16), (((0,), (0,)), ((), ())), preferred_element_type=jnp.float32
    )
    if old is None:
        return top, t, pv
    scale = jnp.exp2(old[0] - top)
    return top, old[1] * scale + t, old[2] * scale + pv


def kernel(
    outer, inner, heads,
    order_hbm, q_hbm, k_hbm, v_hbm, acc, total,
    order, q_ref, kz, kvd, high,
    load_sem, ready, near, zsent, zrecv, sent, recv,
):
    rows, cols = k_hbm.shape
    block = q_ref.shape[0]
    width = kvd.shape[-1]
    q_heads = q_ref.shape[1] // HD
    seq, head = lax.axis_index("seq"), lax.axis_index("head")
    o, j = seq // inner, lax.rem(seq, inner)
    first_heads = max(heads // 2, 1)
    spots = inner * heads
    place = pl.ds(pl.multiple_of(j * block + head * rows, rows), rows)
    inputs = (k_hbm, v_hbm)

    def loop(first, last, body):
        lax.fori_loop(first, last, lambda k, c: (body(k), c)[1], 0)

    def columns(h):
        return pl.ds(pl.multiple_of(h * width, width), width)

    def lane(dj):
        return lax.rem(j + dj, inner)

    def signal(sem, o2, j2, h2):
        pl.semaphore_signal(sem, inc=1, device_id=(o2 * inner + j2, h2), device_id_type=MESH)

    barrier = pltpu.get_barrier_semaphore()

    def each_spot(js, hs, sem):
        def row(j2):
            def one(h2):
                pl.when((j2 != j) | (h2 != head))(lambda: signal(sem, o, j2, h2))
            loop(*hs, one)
        loop(*js, row)

    loop(o + 1, outer, lambda o2: signal(barrier, o2, j, head))
    each_spot((j, inner), (head, heads), barrier)

    own = [
        pltpu.make_async_copy(src.at[:, columns(head)], kvd.at[o, i, place], load_sem.at[0])
        for i, src in enumerate(inputs)
    ]
    qload = pltpu.make_async_copy(q_hbm, q_ref, load_sem.at[1])
    oload = pltpu.make_async_copy(order_hbm, order, load_sem.at[2])
    for c in own + [qload, oload]:
        c.start()

    ahead = o + (j + 1) * (head + 1) - 1
    pl.when(ahead > 0)(lambda: pl.semaphore_wait(barrier, ahead))

    pair = max(heads // 2, 1)

    def zpart(f, size):
        return pl.ds(f * width, size * width)

    def zsend(o2):
        def parts(size):
            for f in range(0, heads, size):
                for i, src in enumerate(inputs):
                    pltpu.make_async_remote_copy(
                        src_ref=src.at[:, zpart(f, size)],
                        dst_ref=kz.at[o, i, :, zpart(f, size)],
                        send_sem=zsent.at[0],
                        recv_sem=zrecv.at[o, f if size == 1 else f + i],
                        device_id=(o2 * inner + j, head),
                        device_id_type=MESH,
                    ).start()

        pl.when(o2 == 0)(lambda: parts(1))
        pl.when(o2 > 0)(lambda: parts(pair))

    loop(0, o, lambda o2: signal(ready.at[o], o2, j, head))

    def piece(ref, src, i, o2, j2, h2, sem):
        pltpu.make_async_remote_copy(
            src_ref=ref.at[:, columns(h2)],
            dst_ref=kvd.at[src, i, place],
            send_sem=sem,
            recv_sem=recv.at[src, j],
            device_id=(o2 * inner + j2, h2),
            device_id_type=MESH,
        ).start()

    loop(0, jnp.minimum(o, 1), zsend)
    each_spot((0, j + 1), (0, head + 1), near.at[0])

    def scatter(src, i, ref, targets):
        for j2, h2 in targets:
            go = (j2 != j) | (h2 != head)
            pl.when(go)(lambda: piece(ref, src, i, o, j2, h2, sent.at[0]))

    def places(f, size, lanes_of=tuple(range(inner))):
        return [(j2, h2) for j2 in lanes_of for h2 in range(f, f + size)]

    every = [(j2, h2) for j2 in range(inner) for h2 in range(heads)]

    def upward(o2):
        pl.semaphore_wait(ready.at[o2], 1)
        zsend(o2)

    def own_scatter():
        above = (inner - j) * (heads - head) - 1
        pl.when(above > 0)(lambda: pl.semaphore_wait(near.at[0], above))
        for i, ref in enumerate(inputs):
            scatter(o, i, ref, every)

    loop(1, o, zsend)
    own_scatter()
    loop(o + 1, outer, upward)

    mine_part = kvd.at[0, :, pl.ds(0, rows)]
    whole = kvd.at[0, :, pl.ds(0, block)]
    part = kvd.at[0, :, pl.ds(0, (heads - 1) * rows)]

    def landed(src, dj):
        ref = whole if dj else part
        pltpu.make_async_copy(ref, ref, recv.at[src, lane(dj)]).wait()

    def arrived(src, f, i, size):
        if size > 1:
            ref = kz.at[0, i, :, zpart(f, size)]
            pltpu.make_async_copy(ref, ref, zrecv.at[src, f + i]).wait()
        elif i == 0:
            ref = kz.at[0, :, :, zpart(f, size)]
            pltpu.make_async_copy(ref, ref, zrecv.at[src, f]).wait()

    def by_plane(body):
        pl.when(o == 0)(lambda: body(1))
        pl.when(o > 0)(lambda: body(pair))

    def keep(src):
        for i in range(2):
            kvd[src, i, place] = kz[src, i, :, columns(head)]

    def pass_on(src, first, size):
        for f in range(first, heads, size):
            for i in range(2):
                arrived(src, f, i, size)
                scatter(src, i, kz.at[src, i], places(f, size))

    def relay(src):
        by_plane(lambda size: pass_on(src, 0, size))

    def relay_pair(*srcs):
        def serve(size):
            late = [(src, f, i) for f in range(0, pair, size) for src in srcs for i in range(2)]
            for src, f, i in late:
                arrived(src, f, i, size)
                scatter(src, i, kz.at[src, i], places(f, size, (0,)))
            for src, f, i in late:
                scatter(src, i, kz.at[src, i], places(f, size, tuple(range(1, inner))))
            for src in srcs:
                pass_on(src, pair, size)

        by_plane(serve)
        for src in srcs:
            keep(src)

    half = max(outer // 2, 1)
    turned = jnp.minimum(o // half, 1)
    seen_from = o + turned * (outer - 1 - 2 * o)

    def source(i):
        a = i + (i + outer - seen_from) // outer
        return a + turned * (outer - 1 - 2 * a)

    lanes = block

    def absorb(blocks, first=False):
        mine = order[seq]
        spots_of = [order[src * inner + l] for src, l in blocks]
        height = len(blocks) * block
        if first:
            row = lax.broadcasted_iota(jnp.int32, (height, lanes), 0)
            col = lax.broadcasted_iota(jnp.int32, (height, lanes), 1)
            start = jnp.full((height, lanes), spots_of[0], jnp.int32) * block
            for l in range(1, len(blocks)):
                start = jnp.where(row >= l * block, (spots_of[l] - l) * block, start)
            mask = mine * block + lax.rem(col, block) >= start + row
        else:
            mask = [jnp.full((1, lanes), spot, jnp.int32) < mine for spot in spots_of]

        def stack(i):
            return jnp.concatenate(
                [kvd[src, i, pl.ds(pl.multiple_of(l * block, block), block)] for src, l in blocks]
            )

        key, value = stack(0), stack(1)
        for g in range(q_heads):
            at = slice(g * block, (g + 1) * block)
            old = None if first else (high[:, at], total[:, at], acc[:, at])
            high[:, at], total[:, at], acc[:, at] = attend(
                q_ref[:, g * HD : (g + 1) * HD], key, value, mask, old
            )

    def both(src):
        for dj in range(inner):
            landed(src, dj)
        return [(src, l) for l in range(inner)]

    qload.wait()
    oload.wait()
    pltpu.make_async_copy(mine_part, mine_part, load_sem.at[0]).wait()
    relayed = outer - 1 if outer <= 8 else 0
    for i in range(relayed - 2):
        relay(source(i))
        keep(source(i))
    if relayed:
        relay_pair(source(relayed - 2), source(relayed - 1))
    absorb(both(o), True)

    def further(i):
        src = source(i)
        if not relayed:
            relay(src)
            keep(src)
        absorb(both(src))

    if relayed:
        for i in range(outer - 3):
            further(i)
    else:
        loop(0, outer - 3, further)
    ends = [source(i) for i in range(outer - 3, outer - 1)]
    if not relayed:
        for src in ends:
            relay(src)
            keep(src)
    front = 1 - jnp.minimum(o, 1)
    near_one, far_one = ends
    landed(near_one, 0)
    pl.when(front == 1)(lambda: landed(far_one, 0))
    pl.when(front == 0)(lambda: landed(near_one, 1))
    turn = front * (far_one - near_one)
    absorb([(near_one, j), (near_one + turn, lane(1) + front * (j - lane(1)))])
    pl.when(front == 1)(lambda: landed(near_one, 1))
    pl.when(front == 0)(lambda: landed(far_one, 0))
    landed(far_one, 1)
    absorb([(far_one - turn, j + front * (lane(1) - j)), (far_one, lane(1))])

    def drained(ref, sem):
        pltpu.make_async_copy(ref, ref, sem).wait()

    drained(kz.at[pl.ds(0, outer - 1)], zsent.at[0])
    scattered = outer * (spots - 1)
    drained(kvd.at[:, :, pl.ds(0, scattered * rows // outer)], sent.at[0])


def finish(acc, total, out_hbm, out, sem):
    block, q_cols = out.shape
    count = sem.shape[0]
    wide = q_cols // count
    copies = []
    for n in range(count):
        for g in range(n * wide // HD, (n + 1) * wide // HD):
            lane = slice(g * block, (g + 1) * block)
            part = acc[:, lane] * (1.0 / total[:, lane])
            out[:, g * HD : (g + 1) * HD] = part.astype(out.dtype).T
        at = pl.ds(n * wide, wide)
        copies.append(pltpu.make_async_copy(out.at[:, at], out_hbm.at[:, at], sem.at[n]))
        copies[-1].start()
    for copy in copies:
        copy.wait()


def local(devices, heads, queries, keys, values, block_order):
    inner = 2 if devices % 2 == 0 else 1
    outer = devices // inner
    rows, cols = keys.shape
    block, q_cols = queries.shape
    width = cols // heads
    assert width == HD and rows * heads == block
    bf16, f32 = jnp.bfloat16, jnp.float32
    lanes = q_cols // HD * block
    assert inner == 2 and outer >= 3 and heads >= 4
    acc, total = pl.pallas_call(
        functools.partial(kernel, outer, inner, heads),
        out_shape=(
            pltpu.VMEM((HD, lanes), f32),
            pltpu.VMEM((1, lanes), f32),
        ),
        in_specs=[pl.BlockSpec(memory_space=pltpu.HBM)] * 4,
        out_specs=[pl.BlockSpec(memory_space=pltpu.VMEM)] * 2,
        scratch_shapes=[
            pltpu.SMEM(block_order.shape, jnp.int32),
            pltpu.VMEM((block, q_cols), bf16),
            pltpu.VMEM((outer, 2, rows, cols), bf16),
            pltpu.VMEM((outer, 2, inner * block, width), bf16),
            pltpu.VMEM((1, lanes), f32),
            pltpu.SemaphoreType.DMA((3,)),
            pltpu.SemaphoreType.REGULAR((outer,)),
            pltpu.SemaphoreType.REGULAR((1,)),
            pltpu.SemaphoreType.DMA((1,)),
            pltpu.SemaphoreType.DMA((outer, heads)),
            pltpu.SemaphoreType.DMA((1,)),
            pltpu.SemaphoreType.DMA((outer, inner)),
        ],
        compiler_params=pltpu.CompilerParams(
            collective_id=0, has_side_effects=True, vmem_limit_bytes=67043328 - 600 * 1024
        ),
    )(block_order, queries, keys, values)
    return pl.pallas_call(
        finish,
        out_shape=jax.ShapeDtypeStruct((block, q_cols), queries.dtype),
        in_specs=[pl.BlockSpec(memory_space=pltpu.VMEM)] * 2,
        out_specs=pl.BlockSpec(memory_space=pltpu.HBM),
        scratch_shapes=[
            pltpu.VMEM((block, q_cols), queries.dtype),
            pltpu.SemaphoreType.DMA((CHUNKS,)),
        ],
        compiler_params=pltpu.CompilerParams(vmem_limit_bytes=8 * 1024 * 1024),
    )(acc, total)


def solution(mesh):
    placed = (P("seq", "head"), P(("seq", "head"), None), P(("seq", "head"), None), P())
    return jax.shard_map(
        functools.partial(local, mesh.shape["seq"], mesh.shape["head"]),
        mesh=mesh, in_specs=placed, out_specs=P("seq", "head"), check_vma=False,
    )
```
